128 devices in a mesh: task: 2 (over core), row: 64 (over x, y, z).
Axes of the slice: x: 4, y: 4, z: 4, core: 2. Of those that a mesh axis runs over, the one named last changes fastest.
Arguments:
- activation_grams: float32 [2, 7168, 7168], P('task', 'row'), may hold values from -240 to 240, as said below
- adjusted_weights: bfloat16 [2, 7168, 2048], P('task', 'row'), may hold values from -0.59765625 to 0.59765625
Outputs:
- reduced_gram: float32 [7168, 7168], P('row')
- reduced_rhs: float32 [7168, 2048], P('row')
The draws below stay inside these ranges and needn't reach their ends.
Inputs may be any that keep to these rules, and one draw needn't show every extreme that they name: Each activation_grams[m] is symmetric and positive definite.
All inputs are finite; a program needn't handle non-finite values.
Results may differ from the reference program's by a relative error of at most 0.0003.
Values may be sent and summed in bfloat16 or wider, within the bound.
A program may use at most 128 MiB of HBM per device.

```python
import math
import jax
import jax.numpy as jnp
from jax import lax

H = 7168
DC = 2048
MODELS = 2
PANEL_STEPS = 2
N_ROW = 64


def draw_activation_grams(key, part):
    loading_key, scale_key = jax.random.split(jax.random.fold_in(key, 11))
    strong_rank = 8
    broad_rank = H + 1024
    base_share = 0.25
    strong_share = 0.5
    broad_share = 0.25
    spread_log = math.log(10.0)
    column_scale = jnp.concatenate([jnp.full((strong_rank,), math.sqrt(strong_share / strong_rank), jnp.float32), jnp.full((broad_rank,), math.sqrt(broad_share / broad_rank), jnp.float32)])

    def one_model(model_key):
        loadings = jax.random.normal(model_key, (H, strong_rank + broad_rank), jnp.float32) * column_scale
        shared = jnp.dot(loadings, loadings.T, precision=lax.Precision.HIGHEST)
        return 0.5 * (shared + shared.T)
    common = lax.map(one_model, jax.random.split(loading_key, MODELS))
    correlated = common + base_share * jnp.eye(H, dtype=jnp.float32)
    position = jnp.arange(H, dtype=jnp.float32) / H
    roughness = jnp.exp(jax.random.uniform(scale_key, (MODELS, H), jnp.float32, 0.0, spread_log))
    rooted = jnp.sqrt(roughness * jnp.exp(math.log(3.0) * position))
    return (rooted[:, :, None] * correlated * rooted[:, None, :]).astype(jnp.float32)


def block_levels(key, shape, pieces, low, largest):
    def one(dim, shards_of):
        steps = jax.random.uniform(jax.random.fold_in(jax.random.fold_in(key, 6), dim), (shards_of,), jnp.float32, low / len(pieces), largest / len(pieces))
        return jnp.repeat(jnp.exp(steps), shape[dim] // shards_of).reshape((-1,) + (1,) * (len(shape) - dim - 1))

    loudness = one(*pieces[0])
    for cut in pieces[1:]:
        loudness = loudness * one(*cut)
    return loudness


def gaussian(stream_key, extent, scale, most, pieces=(), held_as=jnp.bfloat16):
    values = scale * jax.random.normal(stream_key, extent, jnp.float32)
    if pieces:
        values = values * block_levels(stream_key, extent, pieces, -0.22, 0.18)
    return jnp.clip(values, -most, most).astype(held_as)


def setup_inputs(seed: int = 0) -> dict:
    arg_keys = jax.random.split(jax.random.key(seed), 3)
    activation_grams = draw_activation_grams(jax.random.fold_in(arg_keys[2], 71), 0)
    adjusted_weights = gaussian(arg_keys[1], (MODELS, H, DC), 0.1, 0.59765625, ((0, 2), (1, 64)))
    return {"activation_grams": activation_grams, "adjusted_weights": adjusted_weights}


def reference(activation_grams, adjusted_weights):
    rows = H // N_ROW
    merged = jnp.zeros((H, H), jnp.float32)
    rhs = jnp.zeros((H, DC), jnp.float32)
    for model in range(MODELS):
        gram = activation_grams[model]
        diagonal_entries = jnp.diagonal(gram)
        scaling = H / jnp.sum(diagonal_entries)
        regular = scaling * (0.9 * gram + 0.1 * jnp.diag(diagonal_entries))
        merged = merged + regular
        rhs = rhs + jnp.dot(regular, adjusted_weights[model].astype(jnp.float32), precision=lax.Precision.HIGHEST)
    for panel in range(PANEL_STEPS):
        low = panel * rows
        high = low + rows
        factor = jnp.linalg.cholesky(merged[low:high, low:high])
        upper = jax.scipy.linalg.solve_triangular(factor, merged[low:high], lower=True)
        solved = jax.scipy.linalg.solve_triangular(factor, rhs[low:high], lower=True)
        below = upper[:, high:].T
        merged = jnp.concatenate([merged[:low], upper, merged[high:] - jnp.dot(below, upper, precision=lax.Precision.HIGHEST)], axis=0)
        rhs = jnp.concatenate([rhs[:low], solved, rhs[high:] - jnp.dot(below, solved, precision=lax.Precision.HIGHEST)], axis=0)
    return (merged, rhs)
```

```python
import functools

import jax
import jax.numpy as jnp
from jax import lax
from jax.experimental import pallas as pl
from jax.experimental.pallas import tpu as pltpu
from jax.sharding import Mesh
from jax.sharding import PartitionSpec as P

ROW = ("row_0", "row_1", "row_2")
F32 = jnp.float32
BF16 = jnp.bfloat16
B = 112
T = 224
H = 7168
DC = 2048
KX = 1792
HALF = 3584
MESH = pl.DeviceIdType.MESH
HI = lax.Precision.HIGHEST
NCOPY = 176


class Net:
    def __init__(self, send, recv):
        self.send, self.recv, self.n, self.all = send, recv, 0, []

    def copy(self, src, dst, dev, track=True):
        i = self.n
        self.n += 1
        c = pltpu.make_async_remote_copy(
            src_ref=src, dst_ref=dst, send_sem=self.send.at[i], recv_sem=self.recv.at[i],
            device_id=dev, device_id_type=MESH)
        if track:
            self.all.append(c)
        return c

    def go(self, src, dst, dev):
        c = self.copy(src, dst, dev)
        c.start()
        return c


def iota(shape, dim):
    return lax.broadcasted_iota(jnp.int32, shape, dim)


def dot(a, b, dims=((1,), (0,)), precision=None):
    return lax.dot_general(a, b, (dims, ((), ())), precision=precision, preferred_element_type=F32)


def body(a_ref, w_ref, og_ref, or_ref,
         at, bnc, wg, rt, lh, ll, utx, ug, pbuf, prx, sb, rl, rr, rb, fin, finp,
         ah, ap, oh, g, linv, sx, sr, mx, mr, trx, try_, trz, trp, dw, q, send, recv, lsem):
    t = lax.axis_index("task")
    x, y, z = (lax.axis_index(n) for n in ROW)
    p = y * 4 + z
    r = x * 16 + p

    def add(v, d):
        return lax.rem(v + (4 + d), 4)

    def dev(dt=0, dx=0, dy=0, dz=0):
        return (1 - t if dt else t, add(x, dx) if dx else x, add(y, dy) if dy else y, add(z, dz) if dz else z)

    net = Net(send, recv)
    bar = pltpu.get_barrier_semaphore()
    peers = [dev(dt=1)] + [dev(**{a: d}) for a in ("dx", "dy", "dz") for d in (1, -1, 2)]
    for d in peers:
        pl.semaphore_signal(bar, inc=1, device_id=d, device_id_type=MESH)
    pl.semaphore_wait(bar, len(peers))

    ws = (r * 7 // 8 - r // 63) * 128
    ws = pl.multiple_of(ws, 128)
    l_rt = pltpu.make_async_copy(a_ref.at[0, :, 0:256], rt.at[y, z], lsem.at[0])
    l_dw = pltpu.make_async_copy(a_ref.at[0, :, pl.ds(ws, 256)], dw, lsem.at[1])
    l_w = pltpu.make_async_copy(w_ref.at[0], wg.at[y, z], lsem.at[2])
    kx = pl.multiple_of(x * KX, 128)
    l_at = pltpu.make_async_copy(a_ref.at[0, :, pl.ds(kx, KX)], at.at[x], lsem.at[3])
    hc = pl.multiple_of(t * HALF, 128)
    hp = pl.multiple_of((1 - t) * HALF, 128)
    l_ah = pltpu.make_async_copy(a_ref.at[0, :, pl.ds(hc, HALF)], ah, lsem.at[4])
    for c in (l_rt, l_dw, l_w, l_at, l_ah):
        c.start()

    def acol(d):
        return pl.ds(pl.multiple_of(add(x, d) * KX, 128), KX)

    xb = [net.go(a_ref.at[0, 0:56, acol(2)], bnc.at[0], dev(dx=1)),
          net.go(a_ref.at[0, 56:112, acol(2)], bnc.at[1], dev(dx=-1))]
    xd = [net.go(a_ref.at[0, :, acol(1)], at.at[x], dev(dx=1)),
          net.go(a_ref.at[0, :, acol(-1)], at.at[x], dev(dx=-1))]
    xp = net.go(a_ref.at[0, :, pl.ds(hp, HALF)], ap, dev(dt=1))

    def gather(sl, batch):
        def nb(h, stage, d):
            axis = ("dy", "dz")[(h + stage) % 2]
            return dev(**{axis: d})

        def ref(h, part, a, b):
            return sl(h, part, a, b) if h == 0 else sl(h, part, b, a)

        first, second = (y, z), (z, y)
        st = {}

        def ph1(h):
            s = ref(h, None, first[h], second[h])
            st[h, "p"] = net.go(s, s, nb(h, 0, 1))
            st[h, "m"] = net.go(s, s, nb(h, 0, -1))

        def ph2(h, k, a):
            s = ref(h, None, a, second[h])
            st[h, k, "p"] = net.go(s, s, nb(h, 1, 1))
            st[h, k, "m"] = net.go(s, s, nb(h, 1, -1))

        def fw1(h, side):
            d = -1 if side == "p" else 1
            st[h, side].wait_recv()
            s = ref(h, 0 if side == "p" else 1, add(first[h], d), second[h])
            st[h, "f" + side] = net.go(s, s, nb(h, 0, -d))

        def end1(h):
            st[h, "fp"].wait_recv()
            st[h, "fm"].wait_recv()

        def fw2(h, k, a, side):
            d = -1 if side == "p" else 1
            st[h, k, side].wait_recv()
            s = ref(h, 0 if side == "p" else 1, a, add(second[h], d))
            st[h, k, "f" + side] = net.go(s, s, nb(h, 1, -d))

        def end2(h, k):
            st[h, k, "fp"].wait_recv()
            st[h, k, "fm"].wait_recv()

        ev = []
        both = (0, 1)
        if batch:
            every = slice(None)
            ev.append(lambda: [ph1(h) for h in both])
            for side in "pm":
                for h in both:
                    ev.append(functools.partial(fw1, h, side))
            ev.append(lambda: [(end1(h), ph2(h, 0, every)) for h in both])
            for side in "pm":
                for h in both:
                    ev.append(functools.partial(fw2, h, 0, every, side))
            ev.append(lambda: [end2(h, 0) for h in both])
            return ev
        idx = {k: (lambda h, d=d: add(first[h], d) if d else first[h]) for k, d in ((0, 0), (1, -1), (2, 1), (3, 2))}
        ev.append(lambda: ([ph1(h) for h in both], [ph2(h, 0, first[h]) for h in both]))
        for k, side in ((1, "p"), (2, "m")):
            for h in both:
                ev.append(lambda h=h, k=k, side=side: (fw1(h, side), ph2(h, k, idx[k](h))))
        for h in both:
            for side in "pm":
                ev.append(lambda h=h, side=side: fw2(h, 0, idx[0](h), side))
        for h in both:
            ev.append(lambda h=h: (end1(h), ph2(h, 3, idx[3](h))))
        for k in (1, 2, 3):
            for h in both:
                for side in "pm":
                    ev.append(lambda h=h, k=k, side=side: fw2(h, k, idx[k](h), side))
        ev.append(lambda: [end2(h, k) for k in range(4) for h in both])
        return ev

    def sl_rt(h, part, a, b):
        rows = slice(None) if part is None else pl.ds(56 * part, 56)
        return rt.at[a, b, rows, pl.ds(128 * h, 128)]

    def sl_w(h, part, a, b):
        lo, n = (1024 * h, 1024) if part is None else (1024 * h + 512 * part, 512)
        return wg.at[a, b, :, pl.ds(lo, n)]

    def sl_u(h, part, a, b):
        blk = slice(None) if part is None else part
        return ug.at[blk, a, b, :, pl.ds(128 * h, 128)]

    ev_r = gather(sl_rt, True)
    ev_w = gather(sl_w, False)
    ev_u = gather(sl_u, False)

    def pump(ev, n=1):
        for _ in range(min(n, len(ev))):
            ev.pop(0)()

    l_rt.wait()
    pump(ev_r)

    l_dw.wait()
    off = r * B - ws
    tile = iota((B, 256), 1) == iota((B, 256), 0) + off
    part = jnp.sum(jnp.where(tile, dw[...], 0.0), axis=1, keepdims=True)
    part = jnp.sum(part, axis=0, keepdims=True)

    def spread(buf, val, pos, axis):
        buf[pos] = jnp.broadcast_to(val, (8, 128))
        return [net.go(buf.at[pos], buf.at[pos], dev(**{axis: d})) for d in (1, -1, 2)]

    def total(buf, copies):
        for c in copies:
            c.wait_recv()
        return buf[0] + buf[1] + (buf[2] + buf[3])

    cs = spread(trx, part, x, "dx")
    s = total(trx, cs)
    cs = spread(try_, s, y, "dy")
    pump(ev_r, 4)
    s = total(try_, cs)
    cs = spread(trz, s, z, "dz")
    l_w.wait()
    pump(ev_r, 1)
    s = total(trz, cs)
    scale8 = float(H) / s
    trp[0] = scale8
    cp = net.go(trp.at[0], trp.at[1], dev(dt=1))
    pump(ev_r, 4)
    pump(ev_w, 1)
    pump(ev_r, 1)
    scale = scale8[0:1, 0:1]

    lane = iota((B, 256), 1)
    own = rt[y, z]
    hit = lane == iota((B, 256), 0) + r * B
    own = jnp.where(lane < T, own * jnp.where(hit, scale, 0.9 * scale), 0.0)
    mx[...] = own
    cm = net.go(mx, mr, dev(dt=1))
    for i in range(2):
        hit = lane == iota((B, 256), 0) + i * B
        sx[i] = jnp.where(lane < T, rt[0, i] * jnp.where(hit, scale, 0.9 * scale), 0.0)
    cS = net.go(sx, sr, dev(dt=1))
    cp.wait_recv()
    scale_p = trp[1][0:1, 0:1]
    cm.wait_recv()
    cS.wait_recv()

    def chol_steps():
        def start():
            linv[T:256, :] = jnp.zeros((256 - T, 256), F32)
            for i in range(2):
                g[B * i:B * (i + 1), 0:256] = sx[i] + sr[i]
            g[:, 256:512] = jnp.where(iota((T, 256), 0) == iota((T, 256), 1), 1.0, 0.0)

        def step(b):
            k0 = 16 * b
            rr_ = g[k0:k0 + 16, :]
            rid = iota((16, 1), 0)
            for j in range(16):
                row = rr_[j:j + 1, :]
                col = rr_[:, k0 + j:k0 + j + 1]
                inv = 1.0 / row[:, k0 + j:k0 + j + 1]
                rr_ = rr_ - jnp.where(rid > j, col * inv, 0.0) * row
            dg = jnp.sum(jnp.where(iota((16, 512), 1) == iota((16, 512), 0) + k0, rr_, 0.0), axis=1, keepdims=True)
            rr_ = rr_ * (1.0 / jnp.sqrt(dg))
            linv[k0:k0 + 16, :] = rr_[:, 256:512]
            if b < 13:
                left = jnp.where(iota((16, 256), 1) >= k0 + 16, rr_[:, 0:256], 0.0)
                upd = dot(left, rr_, ((0,), (0,)), HI)
                g[k0 + 16:T, :] = g[k0 + 16:T, :] - upd[k0 + 16:T, :]

        return [start] + [functools.partial(step, b) for b in range(14)]

    for f in chol_steps():
        pl.when(x == 0)(f)
        pump(ev_w, 1)
    lc = [net.copy(linv, linv, dev(dx=d), track=False) for d in (1, 2, -1)]

    @pl.when(x == 0)
    def _():
        for c in lc:
            c.start()
        for c in lc:
            c.wait_send()

    for i, c in enumerate(lc):
        @pl.when(x == (1, 2, 3)[i])
        def _(c=c):
            c.wait_recv()

    ut = dot(mx[...] + mr[...], linv[...], ((1,), (1,)), HI)
    utx[x] = ut
    cu = [net.go(utx.at[x], utx.at[x], dev(dx=d)) for d in (1, -1, 2)]
    pump(ev_w, 2)
    xb[0].wait_recv()
    f0 = net.go(bnc.at[0], at.at[add(x, -1), 0:56], dev(dx=1))
    xb[1].wait_recv()
    f1 = net.go(bnc.at[1], at.at[add(x, 1), 56:112], dev(dx=-1))
    for c in cu:
        c.wait_recv()
    for i in range(2):
        ug[i, y, z] = utx[2 * t + i]
    pump(ev_u, 1)
    pump(ev_w, 99)
    for c in xd + [f0, f1]:
        c.wait_recv()
    l_at.wait()

    def split(v):
        hi = v.astype(BF16)
        return hi, (v - hi.astype(F32)).astype(BF16)

    for i in range(4):
        v = at[i]
        same = (i == x).astype(jnp.int32)
        hit = iota((B, KX), 1) == iota((B, KX), 0) + (p * B + (1 - same) * H)
        v = v * jnp.where(hit, 1.0, 0.9)
        lh[B * i:B * (i + 1), :], ll[B * i:B * (i + 1), :] = split(v)
    v = rt[...].reshape(KX, 256)
    hit = iota((KX, 256), 0) + x * KX == iota((KX, 256), 1)
    v = jnp.where(iota((KX, 256), 1) < T, v * jnp.where(hit, 1.0, 0.9), 0.0)
    v = v.T
    lh[448:704, :], ll[448:704, :] = split(v)

    top = (p < 2).astype(F32)
    sel = jnp.where(iota((B, 256), 1) == iota((B, 256), 0) + p * B, -1.0, 0.0)
    q[0] = utx[0] * (1.0 - top) + sel * top
    for i in range(1, 4):
        q[i] = utx[i]

    cd = []
    for j in range(8):
        n = lax.rem((1 - t) * 4 + j, 8)
        wcol = wg[:, :, :, pl.ds(pl.multiple_of(n * 256, 256), 256)].reshape(KX, 256)
        acc = dot(lh[...], wcol) + dot(ll[...], wcol)
        yv = dot(linv[...], acc[448:704], precision=HI)
        cor = dot(q[...].reshape(448, 256), yv, precision=HI)
        for i in range(4):
            pc = acc[B * i:B * (i + 1)]
            if i == 0:
                pc = pc * (1.0 - top)
            pbuf[j, i] = (pc - cor[B * i:B * (i + 1)]) * scale
        if j < 4:
            cd.append(net.go(pbuf.at[j], prx.at[j], dev(dt=1)))
        pump(ev_u, 3)
    for j in range(4):
        cd[j].wait_recv()
        for i in range(4):
            sb[i, j] = pbuf[4 + j, i] + prx[j, i]

    o = add(x, 2)
    r0 = net.go(sb.at[o, 0:2], rl, dev(dx=1))
    r1 = net.go(sb.at[o, 2:4], rr, dev(dx=-1))
    r0.wait_recv()
    xn = add(x, 1)
    sb[xn, 0:2] = sb[xn, 0:2] + rl[...]
    r2 = net.go(sb.at[xn], rb.at[0], dev(dx=1))
    r1.wait_recv()
    xm = add(x, -1)
    sb[xm, 2:4] = sb[xm, 2:4] + rr[...]
    r3 = net.go(sb.at[xm], rb.at[1], dev(dx=-1))
    pump(ev_u, 99)

    l_ah.wait()
    xp.wait_recv()
    topr = (r < 2).astype(F32)
    selr = jnp.where(iota((B, 256), 1) == iota((B, 256), 0) + r * B, -1.0, 0.0)
    qc = utx[x] * (1.0 - topr) + selr * topr
    keep = 1.0 - topr
    lcp = []
    for i in range(2):
        for c in range(7):
            cc = i * 7 + c
            cols = slice(cc * 256, (cc + 1) * 256)
            u = ug[i].reshape(KX, 256)[c * 256:(c + 1) * 256]
            hit = iota((B, 256), 1) + (cc * 256) == iota((B, 256), 0) + (r * B - t * HALF)
            m = ah[:, cols] * (scale * keep) + ap[:, cols] * (scale_p * keep)
            oh[:, cols] = m * jnp.where(hit, 1.0, 0.9) - dot(qc, u, ((1,), (1,)), HI)
    co = pltpu.make_async_copy(oh, og_ref.at[:, pl.ds(hc, HALF)], lsem.at[5])
    co.start()
    cg = net.go(oh, og_ref.at[:, pl.ds(hc, HALF)], dev(dt=1))

    r2.wait_recv()
    r3.wait_recv()
    fin[...] = sb[x] + (rb[0] + rb[1])
    cf = net.go(fin, finp, dev(dt=1))
    cf.wait_recv()
    for j in range(4):
        or_ref[:, pl.ds(pl.multiple_of(t * 1024 + 256 * j, 256), 256)] = fin[j]
        or_ref[:, pl.ds(pl.multiple_of((1 - t) * 1024 + 256 * j, 256), 256)] = finp[j]
    co.wait()
    cg.wait_recv()
    for c in net.all:
        c.wait_send()
    assert net.n <= NCOPY, net.n


def per_device(grams, weights):
    V = pltpu.VMEM
    scratch = [
        V((4, B, KX), F32), V((2, 56, KX), F32), V((4, 4, B, DC), BF16), V((4, 4, B, 256), F32),
        V((704, KX), BF16), V((704, KX), BF16), V((4, B, 256), F32), V((2, 4, 4, B, 256), F32),
        V((8, 4, B, 256), F32), V((4, 4, B, 256), F32), V((4, 4, B, 256), F32),
        V((2, B, 256), F32), V((2, B, 256), F32), V((2, 4, B, 256), F32), V((4, B, 256), F32), V((4, B, 256), F32),
        V((B, HALF), F32), V((B, HALF), F32), V((B, HALF), F32), V((T, 512), F32), V((256, 256), F32),
        V((2, B, 256), F32), V((2, B, 256), F32), V((B, 256), F32), V((B, 256), F32),
        V((4, 8, 128), F32), V((4, 8, 128), F32), V((4, 8, 128), F32), V((2, 8, 128), F32),
        V((B, 256), F32), V((4, B, 256), F32),
        pltpu.SemaphoreType.DMA((NCOPY,)), pltpu.SemaphoreType.DMA((NCOPY,)), pltpu.SemaphoreType.DMA((8,)),
    ]
    return pl.pallas_call(
        body,
        out_shape=(jax.ShapeDtypeStruct((B, H), F32), jax.ShapeDtypeStruct((B, DC), F32)),
        in_specs=[pl.BlockSpec(memory_space=pl.ANY)] * 2,
        out_specs=(pl.BlockSpec(memory_space=pl.ANY), pl.BlockSpec(memory_space=pltpu.VMEM)),
        scratch_shapes=scratch,
        compiler_params=pltpu.CompilerParams(
            collective_id=0, has_side_effects=True, vmem_limit_bytes=62 * 1024 * 1024),
    )(grams, weights)


def solution(mesh):
    torus = Mesh(mesh.devices.reshape(mesh.shape["task"], 4, 4, 4), ("task",) + ROW)
    return jax.shard_map(
        per_device, mesh=torus, in_specs=(P("task", ROW, None), P("task", ROW, None)),
        out_specs=(P(ROW, None), P(ROW, None)), check_vma=False)
```

```python
import functools

import jax
import jax.numpy as jnp
from jax import lax
from jax.experimental import pallas as pl
from jax.experimental.pallas import tpu as pltpu
from jax.sharding import Mesh
from jax.sharding import PartitionSpec as P

ROW = ("row_0", "row_1", "row_2")
F32 = jnp.float32
BF16 = jnp.bfloat16
B = 112
T = 224
H = 7168
DC = 2048
KX = 1792
HALF = 3584
MESH = pl.DeviceIdType.MESH
HI = lax.Precision.HIGHEST
NCOPY = 208


class Net:
    def __init__(self, send, recv):
        self.send, self.recv, self.n, self.all = send, recv, 0, []

    def copy(self, src, dst, dev, track=True):
        i = self.n
        self.n += 1
        c = pltpu.make_async_remote_copy(
            src_ref=src, dst_ref=dst, send_sem=self.send.at[i], recv_sem=self.recv.at[i],
            device_id=dev, device_id_type=MESH)
        if track:
            self.all.append(c)
        return c

    def go(self, src, dst, dev):
        c = self.copy(src, dst, dev)
        c.start()
        return c


def iota(shape, dim):
    return lax.broadcasted_iota(jnp.int32, shape, dim)


def dot(a, b, dims=((1,), (0,)), precision=None):
    return lax.dot_general(a, b, (dims, ((), ())), precision=precision, preferred_element_type=F32)


def split(v):
    hi = v.astype(BF16)
    return hi, (v - hi.astype(F32)).astype(BF16)


def dot3(a, b, dims=((1,), (0,))):
    return dot(a[0], b[0], dims) + (dot(a[0], b[1], dims) + dot(a[1], b[0], dims))


def chol_steps(g, linv, corner):
    nb = 32

    def start():
        linv[T:256, 0:128] = jnp.zeros((256 - T, 128), F32)
        linv[T:256, 128:256] = jnp.zeros((256 - T, 128), F32)
        for i in range(2):
            g[B * i:B * (i + 1), 0:256] = corner(i)
        g[:, 256:512] = jnp.where(iota((T, 256), 0) == iota((T, 256), 1), 1.0, 0.0)

    def step(b):
        rid = iota((nb, 128), 0)
        k0 = nb * b
        left = [i for i in (0, 1) if 128 * (i + 1) > k0]
        tiles = left + [2] + ([3] if k0 + nb > 128 else [])
        v = {i: g[k0:k0 + nb, 128 * i:128 * i + 128] for i in tiles}

        def column(k):
            i = k // 128
            return jnp.broadcast_to(v[i][:, k % 128:k % 128 + 1], (nb, 128))

        for j in range(0, nb, 2):
            c0, c1 = column(k0 + j), column(k0 + j + 1)
            d00, d01, d11 = c0[j:j + 1], c1[j:j + 1], c1[j + 1:j + 2]
            inv = 1.0 / (d00 * d11 - d01 * d01)
            f0 = jnp.where(rid > j + 1, (d11 * inv) * c0 - (d01 * inv) * c1, 0.0)
            f1 = jnp.where(rid > j + 1, (d00 * inv) * c1 - (d01 * inv) * c0, 0.0)
            f0 = jnp.where(rid == j + 1, d01 / d00, f0)
            for i in tiles:
                v[i] = v[i] - f0 * v[i][j:j + 1, :] - f1 * v[i][j + 1:j + 2, :]
        dg = 0.0
        for i in left:
            dg = dg + jnp.sum(jnp.where(iota((nb, 128), 1) + 128 * i == rid + k0, v[i], 0.0), axis=1, keepdims=True)
        sc = 1.0 / jnp.sqrt(dg)
        for i in tiles:
            v[i] = v[i] * sc
        linv[k0:k0 + nb, 0:128] = v[2]
        if 3 in v:
            linv[k0:k0 + nb, 128:256] = v[3]
        if k0 + nb < T:
            lo = 128 if k0 + nb >= 128 else 0
            lhs = jnp.concatenate([v[i] for i in left if 128 * i >= lo], axis=1)
            off = k0 + nb - lo
            for i in tiles:
                if 128 * (i + 1) > lo:
                    cols = slice(128 * i, 128 * i + 128)
                    upd = dot(lhs, v[i], ((0,), (0,)), HI)
                    g[k0 + nb:T, cols] = g[k0 + nb:T, cols] - upd[off:off + T - k0 - nb, :]

    return [start] + [functools.partial(step, b) for b in range(T // nb)]


def body(a_ref, w_ref, og_ref, or_ref,
         at, bnc, wg, rt, lh, ll, mxx, q, ug, pbuf, prx, sb, rlr, rb, fin, finp,
         ah, ap, oh, g, linv, sx, sr, mx, mr, trx, try_, trz, trp, dw, send, recv, lsem):
    t = lax.axis_index("task")
    x, y, z = (lax.axis_index(n) for n in ROW)
    p = y * 4 + z
    r = x * 16 + p

    def add(v, d):
        return lax.rem(v + (4 + d), 4)

    def dev(dt=0, dx=0, dy=0, dz=0):
        return (1 - t if dt else t, add(x, dx) if dx else x, add(y, dy) if dy else y, add(z, dz) if dz else z)

    net = Net(send, recv)
    ws = pl.multiple_of((r * 7 // 8 - r // 63) * 128, 128)
    kx = pl.multiple_of(x * KX, 128)
    hc = pl.multiple_of(t * HALF, 128)
    hp = pl.multiple_of((1 - t) * HALF, 128)
    loads = [(a_ref.at[0, :, pl.ds(ws, 256)], dw), (a_ref.at[0, :, 0:256], rt.at[y, z]), (w_ref.at[0], wg.at[y, z]),
             (a_ref.at[0, :, pl.ds(kx, KX)], at.at[x]), (a_ref.at[0, :, pl.ds(hc, HALF)], ah)]
    loads = [pltpu.make_async_copy(a, b, lsem.at[i]) for i, (a, b) in enumerate(loads)]
    l_dw, l_rt, l_w, l_at, l_ah = loads
    for c in loads:
        c.start()
    bar = pltpu.get_barrier_semaphore()
    peers = [dev(dt=1)] + [dev(**{a: d}) for a in ("dx", "dy", "dz") for d in (1, -1, 2)]
    for d in peers:
        pl.semaphore_signal(bar, inc=1, device_id=d, device_id_type=MESH)
    pl.semaphore_wait(bar, len(peers))

    def spread(buf, val, pos, axis):
        buf[pos] = jnp.broadcast_to(val, (8, 128))
        return [net.go(buf.at[pos], buf.at[pos], dev(**{axis: d})) for d in (1, -1, 2)]

    def total(buf, copies):
        for c in copies:
            c.wait_recv()
        return buf[0] + buf[1] + (buf[2] + buf[3])

    def gather(sl, batch):
        def nb(h, stage, d):
            axis = ("dy", "dz")[(h + stage) % 2]
            return dev(**{axis: d})

        def ref(h, part, a, b):
            return sl(h, part, a, b) if h == 0 else sl(h, part, b, a)

        first, second = (y, z), (z, y)
        st = {}

        def ph1(h):
            s = ref(h, None, first[h], second[h])
            st[h, "p"] = net.go(s, s, nb(h, 0, 1))
            st[h, "m"] = net.go(s, s, nb(h, 0, -1))

        def ph2(h, k, a):
            s = ref(h, None, a, second[h])
            st[h, k, "p"] = net.go(s, s, nb(h, 1, 1))
            st[h, k, "m"] = net.go(s, s, nb(h, 1, -1))

        def fw1(h, side):
            d = -1 if side == "p" else 1
            st[h, side].wait_recv()
            s = ref(h, 0 if side == "p" else 1, add(first[h], d), second[h])
            st[h, "f" + side] = net.go(s, s, nb(h, 0, -d))

        def end1(h):
            st[h, "fp"].wait_recv()
            st[h, "fm"].wait_recv()

        def fw2(h, k, a, side):
            d = -1 if side == "p" else 1
            st[h, k, side].wait_recv()
            s = ref(h, 0 if side == "p" else 1, a, add(second[h], d))
            st[h, k, "f" + side] = net.go(s, s, nb(h, 1, -d))

        def end2(h, k):
            st[h, k, "fp"].wait_recv()
            st[h, k, "fm"].wait_recv()

        ev = []
        both = (0, 1)
        if batch:
            every = slice(None)
            ev.append(lambda: [ph1(h) for h in both])
            for side in "pm":
                for h in both:
                    ev.append(functools.partial(fw1, h, side))
            ev.append(lambda: [(end1(h), ph2(h, 0, every)) for h in both])
            for side in "pm":
                for h in both:
                    ev.append(functools.partial(fw2, h, 0, every, side))
            ev.append(lambda: [end2(h, 0) for h in both])
            return ev
        idx = {k: (lambda h, d=d: add(first[h], d) if d else first[h]) for k, d in ((0, 0), (1, -1), (2, 1), (3, 2))}
        ev.append(lambda: ([ph1(h) for h in both], [ph2(h, 0, first[h]) for h in both]))
        for k, side in ((1, "p"), (2, "m")):
            for h in both:
                ev.append(lambda h=h, k=k, side=side: (fw1(h, side), ph2(h, k, idx[k](h))))
        for h in both:
            for side in "pm":
                ev.append(lambda h=h, side=side: fw2(h, 0, idx[0](h), side))
        for h in both:
            ev.append(lambda h=h: (end1(h), ph2(h, 3, idx[3](h))))
        for k in (1, 2, 3):
            for h in both:
                for side in "pm":
                    ev.append(lambda h=h, k=k, side=side: fw2(h, k, idx[k](h), side))
        ev.append(lambda: [end2(h, k) for k in range(4) for h in both])
        return ev

    def sl_rt(h, part, a, b):
        rows = slice(None) if part is None else pl.ds(56 * part, 56)
        return rt.at[a, b, rows, pl.ds(128 * h, 128)]

    def sl_w(k, h, part, a, b):
        lo, n = (1024 * h + 512 * k, 512) if part is None else (1024 * h + 512 * k + 256 * part, 256)
        return wg.at[a, b, :, pl.ds(lo, n)]

    def sl_u(h, part, a, b):
        blk = slice(None) if part is None else part
        return ug.at[blk, a, b, :, pl.ds(128 * h, 128)]

    ev_r = gather(sl_rt, True)
    ev_w = [gather(functools.partial(sl_w, k), False) for k in range(2)]
    ev_u = gather(sl_u, False)

    def pump(ev, n=1):
        for _ in range(min(n, len(ev))):
            ev.pop(0)()

    l_rt.wait()
    pump(ev_r)
    l_dw.wait()
    tile = iota((B, 256), 1) == iota((B, 256), 0) + (r * B - ws)
    part = jnp.sum(jnp.where(tile, dw[...], 0.0), axis=1, keepdims=True)
    part = jnp.sum(part, axis=0, keepdims=True)
    cs = spread(trx, part, x, "dx")

    def acol(d):
        return pl.ds(pl.multiple_of(add(x, d) * KX, 128), KX)

    xb = [net.go(a_ref.at[0, 0:56, acol(2)], bnc.at[0], dev(dx=1)),
          net.go(a_ref.at[0, 56:112, acol(2)], bnc.at[1], dev(dx=-1))]
    xd = [net.go(a_ref.at[0, :, acol(1)], at.at[x], dev(dx=1)),
          net.go(a_ref.at[0, :, acol(-1)], at.at[x], dev(dx=-1))]
    xp = net.go(a_ref.at[0, :, pl.ds(hp, HALF)], ap, dev(dt=1))
    xf = []

    def relay0():
        xb[0].wait_recv()
        xf.append(net.go(bnc.at[0], at.at[add(x, -1), 0:56], dev(dx=1)))

    def relay1():
        xb[1].wait_recv()
        xf.append(net.go(bnc.at[1], at.at[add(x, 1), 56:112], dev(dx=-1)))

    ev_a = [relay0, relay1]

    s = total(trx, cs)
    cs = spread(try_, s, y, "dy")
    pump(ev_r, 4)
    s = total(try_, cs)
    cs = spread(trz, s, z, "dz")
    pump(ev_r, 1)
    s = total(trz, cs)
    scale8 = float(H) / s
    trp[0] = scale8
    cp = net.go(trp.at[0], trp.at[1], dev(dt=1))
    scale = scale8[0:1, 0:1]
    pump(ev_r, 4)
    l_w.wait()
    pump(ev_w[0], 1)
    pump(ev_r, 1)

    lane = iota((B, 256), 1)
    hit = lane == iota((B, 256), 0) + r * B
    mx[...] = jnp.where(lane < T, rt[y, z] * jnp.where(hit, scale, 0.9 * scale), 0.0)
    cm = net.go(mx, mr, dev(dt=1))
    for i in range(2):
        hit = lane == iota((B, 256), 0) + i * B
        sx[i] = jnp.where(lane < T, rt[0, i] * jnp.where(hit, scale, 0.9 * scale), 0.0)
    cS = net.go(sx, sr, dev(dt=1))
    cp.wait_recv()
    scale_p = trp[1][0:1, 0:1]
    cm.wait_recv()
    mxx[x] = mx[...] + mr[...]
    cu = [net.go(mxx.at[x], mxx.at[x], dev(dx=d)) for d in (1, -1, 2)]
    pump(ev_a, 2)
    cS.wait_recv()

    for f in chol_steps(g, linv, lambda i: sx[i] + sr[i]):
        pl.when(x == 0)(f)
        pump(ev_w[0], 2)

    lo, hi = linv.at[0:T, 0:128], linv.at[128:T, 128:256]
    lc = [[net.copy(v, v, dev(dx=d), track=False) for v in (lo, hi)] for d in (1, 2, -1)]

    @pl.when(x == 0)
    def _():
        linv[0:128, 128:256] = jnp.zeros((128, 128), F32)
        for cc in lc:
            for c in cc:
                c.start()

    @pl.when(x > 0)
    def _():
        linv[T:256, :] = jnp.zeros((256 - T, 256), F32)
        linv[0:128, 128:256] = jnp.zeros((128, 128), F32)

    v = rt[...].reshape(KX, 256)
    hit = iota((KX, 256), 0) + x * KX == iota((KX, 256), 1)
    v = jnp.where(iota((KX, 256), 1) < T, v * jnp.where(hit, 1.0, 0.9), 0.0)
    v = v.T
    lh[448:704, :], ll[448:704, :] = split(v)

    pump(ev_w[0], 99)
    pump(ev_w[1], 1)
    for c in xd + xf:
        c.wait_recv()
    l_at.wait()
    for i in range(4):
        v = at[i]
        same = (i == x).astype(jnp.int32)
        hit = iota((B, KX), 1) == iota((B, KX), 0) + (p * B + (1 - same) * H)
        v = v * jnp.where(hit, 1.0, 0.9)
        lh[B * i:B * (i + 1), :], ll[B * i:B * (i + 1), :] = split(v)

    for c in cu:
        c.wait_recv()

    for i, cc in enumerate(lc):
        @pl.when(x == (1, 2, 3)[i])
        def _(cc=cc):
            for c in cc:
                c.wait_recv()

    lin = split(linv[...])
    top = (p < 2).astype(F32)
    sel = jnp.where(iota((B, 256), 1) == iota((B, 256), 0) + p * B, -1.0, 0.0)
    ut = dot3(split(mxx[...].reshape(448, 256)), lin, ((1,), (1,)))
    for i in range(4):
        q[i] = ut[B * i:B * (i + 1)]
    for i in range(2):
        ug[i, y, z] = q[2 * t + i]
    topr = (r < 2).astype(F32)
    selr = jnp.where(iota((B, 256), 1) == iota((B, 256), 0) + r * B, -1.0, 0.0)
    qc = split(q[x] * (1.0 - topr) + selr * topr)
    q[0] = q[0] * (1.0 - top) + sel * top
    qg = split(q[...].reshape(448, 256))

    def product(k, j):
        n = (1 - t if j < 2 else t) * 4 + k * 2 + j % 2
        wcol = wg[:, :, :, pl.ds(pl.multiple_of(n * 256, 256), 256)].reshape(KX, 256)
        acc = dot(lh[...], wcol) + dot(ll[...], wcol)
        yv = dot3(lin, split(acc[448:704]))
        cor = dot3(qg, split(yv))
        for i in range(4):
            pc = acc[B * i:B * (i + 1)]
            if i == 0:
                pc = pc * (1.0 - top)
            pbuf[k, j, i] = (pc - cor[B * i:B * (i + 1)]) * scale

    rs = {}

    def pair_send(k, j):
        rs[k, "d", j] = net.go(pbuf.at[k, j], prx.at[k, j], dev(dt=1))

    xo, xn, xm = add(x, 2), add(x, 1), add(x, -1)

    def rs0(k):
        for j in range(2):
            rs[k, "d", j].wait_recv()
            for i in range(4):
                sb[k, i, j] = pbuf[k, 2 + j, i] + prx[k, j, i]
        rs[k, 0] = net.go(sb.at[k, xo, 0], rlr.at[k, 0], dev(dx=1))
        rs[k, 1] = net.go(sb.at[k, xo, 1], rlr.at[k, 1], dev(dx=-1))

    def rs1(k):
        rs[k, 0].wait_recv()
        sb[k, xn, 0] = sb[k, xn, 0] + rlr[k, 0]
        rs[k, 2] = net.go(sb.at[k, xn], rb.at[k, 0], dev(dx=1))
        rs[k, 1].wait_recv()
        sb[k, xm, 1] = sb[k, xm, 1] + rlr[k, 1]
        rs[k, 3] = net.go(sb.at[k, xm], rb.at[k, 1], dev(dx=-1))

    def rs2(k):
        rs[k, 2].wait_recv()
        rs[k, 3].wait_recv()
        fin[k] = sb[k, x] + (rb[k, 0] + rb[k, 1])
        rs[k, 4] = net.go(fin.at[k], finp.at[k], dev(dt=1))

    def rs3(k):
        rs[k, 4].wait_recv()
        for j in range(2):
            or_ref[:, pl.ds(pl.multiple_of(t * 1024 + k * 512 + 256 * j, 256), 256)] = fin[k, j]
            or_ref[:, pl.ds(pl.multiple_of((1 - t) * 1024 + k * 512 + 256 * j, 256), 256)] = finp[k, j]

    for j in range(4):
        product(0, j)
        if j < 2:
            pair_send(0, j)
        pump(ev_w[1], 3)
    rs0(0)
    pump(ev_w[1], 2)
    pump(ev_u, 1)
    l_ah.wait()
    xp.wait_recv()
    keep = 1.0 - topr
    hit = iota((B, HALF), 1) == iota((B, HALF), 0) + (r * B - t * HALF)
    m = ah[...] * (scale * keep) + ap[...] * (scale_p * keep)
    oh[...] = m * jnp.where(hit, 1.0, 0.9)
    rs1(0)
    pump(ev_w[1], 99)
    for j in range(4):
        product(1, j)
        if j < 2:
            pair_send(1, j)
        pump(ev_u, 3)
        if j == 2:
            rs2(0)
    rs0(1)
    pump(ev_u, 4)
    rs3(0)
    rs1(1)
    pump(ev_u, 99)
    out = []
    for i in range(2):
        for c in range(7):
            cols = slice((i * 7 + c) * 256, (i * 7 + c + 1) * 256)
            u = split(ug[i].reshape(KX, 256)[c * 256:(c + 1) * 256])
            oh[:, cols] = oh[:, cols] - dot3(qc, u, ((1,), (1,)))
        src = oh.at[:, i * KX:(i + 1) * KX]
        dst = og_ref.at[:, pl.ds(pl.multiple_of(t * HALF + i * KX, 128), KX)]
        co = pltpu.make_async_copy(src, dst, lsem.at[5 + i])
        co.start()
        out.append((co, net.go(src, dst, dev(dt=1))))
    rs2(1)
    rs3(1)
    for co, cg in out:
        co.wait()
        cg.wait_recv()
    for c in net.all:
        c.wait_send()

    @pl.when(x == 0)
    def _():
        for cc in lc:
            for c in cc:
                c.wait_send()
    assert net.n <= NCOPY, net.n


def per_device(grams, weights):
    V = pltpu.VMEM
    scratch = [
        V((4, B, KX), F32), V((2, 56, KX), F32), V((4, 4, B, DC), BF16), V((4, 4, B, 256), F32),
        V((704, KX), BF16), V((704, KX), BF16), V((4, B, 256), F32), V((4, B, 256), F32), V((2, 4, 4, B, 256), F32),
        V((2, 4, 4, B, 256), F32), V((2, 2, 4, B, 256), F32), V((2, 4, 2, B, 256), F32),
        V((2, 2, B, 256), F32), V((2, 2, 2, B, 256), F32), V((2, 2, B, 256), F32), V((2, 2, B, 256), F32),
        V((B, HALF), F32), V((B, HALF), F32), V((B, HALF), F32), V((T, 512), F32), V((256, 256), F32),
        V((2, B, 256), F32), V((2, B, 256), F32), V((B, 256), F32), V((B, 256), F32),
        V((4, 8, 128), F32), V((4, 8, 128), F32), V((4, 8, 128), F32), V((2, 8, 128), F32), V((B, 256), F32),
        pltpu.SemaphoreType.DMA((NCOPY,)), pltpu.SemaphoreType.DMA((NCOPY,)), pltpu.SemaphoreType.DMA((8,)),
    ]
    return pl.pallas_call(
        body,
        out_shape=(jax.ShapeDtypeStruct((B, H), F32), jax.ShapeDtypeStruct((B, DC), F32)),
        in_specs=[pl.BlockSpec(memory_space=pl.ANY)] * 2,
        out_specs=(pl.BlockSpec(memory_space=pl.ANY), pl.BlockSpec(memory_space=pltpu.VMEM)),
        scratch_shapes=scratch,
        compiler_params=pltpu.CompilerParams(
            collective_id=0, has_side_effects=True, vmem_limit_bytes=62 * 1024 * 1024),
    )(grams, weights)


def solution(mesh):
    torus = Mesh(mesh.devices.reshape(mesh.shape["task"], 4, 4, 4), ("task",) + ROW)
    return jax.shard_map(
        per_device, mesh=torus, in_specs=(P("task", ROW, None), P("task", ROW, None)),
        out_specs=(P(ROW, None), P(ROW, None)), check_vma=False)
```

```python
import functools

import jax
import jax.numpy as jnp
from jax import lax
from jax.experimental import pallas as pl
from jax.experimental.pallas import tpu as pltpu
from jax.sharding import Mesh
from jax.sharding import PartitionSpec as P

ROW = ("row_0", "row_1", "row_2")
F32 = jnp.float32
BF16 = jnp.bfloat16
B = 112
T = 224
H = 7168
DC = 2048
KX = 1792
HALF = 3584
MESH = pl.DeviceIdType.MESH
HI = lax.Precision.HIGHEST
NCOPY = 216
NSEND = 200
CHUNKS = (512, 512)
NK = len(CHUNKS)


class Net:
    def __init__(self, send, recv):
        self.send, self.recv, self.n, self.all, self.sends, self.free = send, recv, 0, [], 0, []

    def copy(self, src, dst, dev, track=True, like=None):
        i = self.n
        self.n += 1
        k = i if like is None else like
        if self.free:
            j = self.free.pop()
        else:
            j = self.sends
            self.sends += 1
        c = pltpu.make_async_remote_copy(
            src_ref=src, dst_ref=dst, send_sem=self.send.at[j], recv_sem=self.recv.at[k],
            device_id=dev, device_id_type=MESH)
        if track:
            self.all.append((c, j))
        return c

    def retire(self, n):
        for c, j in self.all[:n]:
            c.wait_send()
            self.free.append(j)
        del self.all[:n]

    def go(self, src, dst, dev):
        c = self.copy(src, dst, dev)
        c.start()
        return c


def iota(shape, dim):
    return lax.broadcasted_iota(jnp.int32, shape, dim)


def dot(a, b, dims=((1,), (0,)), precision=None):
    return lax.dot_general(a, b, (dims, ((), ())), precision=precision, preferred_element_type=F32)


def split(v):
    hi = v.astype(BF16)
    return hi, (v - hi.astype(F32)).astype(BF16)


def dot3(a, b, dims=((1,), (0,))):
    return dot(a[0], b[0], dims) + (dot(a[0], b[1], dims) + dot(a[1], b[0], dims))


GROUPS = dict(opp=(0, B, 592), z=(224, 256, 0), p1=(736, B, 368), m1=(960, B, 480), own=(1184, B, 256))


def chol_steps(g, linv, corner):
    nb = 32

    def start():
        linv[T:256, 0:128] = jnp.zeros((256 - T, 128), F32)
        linv[T:256, 128:256] = jnp.zeros((256 - T, 128), F32)
        for i in range(2):
            g[B * i:B * (i + 1), 0:256] = corner(i)
        g[:, 256:512] = jnp.where(iota((T, 256), 0) == iota((T, 256), 1), 1.0, 0.0)

    def step(b):
        rid = iota((nb, 128), 0)
        k0 = nb * b
        left = [i for i in (0, 1) if 128 * (i + 1) > k0]
        tiles = left + [2] + ([3] if k0 + nb > 128 else [])
        v = {i: g[k0:k0 + nb, 128 * i:128 * i + 128] for i in tiles}

        def column(k):
            i = k // 128
            return jnp.broadcast_to(v[i][:, k % 128:k % 128 + 1], (nb, 128))

        for j in range(0, nb, 2):
            c0, c1 = column(k0 + j), column(k0 + j + 1)
            d00, d01, d11 = c0[j:j + 1], c1[j:j + 1], c1[j + 1:j + 2]
            inv = 1.0 / (d00 * d11 - d01 * d01)
            f0 = jnp.where(rid > j + 1, (d11 * inv) * c0 - (d01 * inv) * c1, 0.0)
            f1 = jnp.where(rid > j + 1, (d00 * inv) * c1 - (d01 * inv) * c0, 0.0)
            f0 = jnp.where(rid == j + 1, d01 / d00, f0)
            for i in tiles:
                v[i] = v[i] - f0 * v[i][j:j + 1, :] - f1 * v[i][j + 1:j + 2, :]
        dg = 0.0
        for i in left:
            dg = dg + jnp.sum(jnp.where(iota((nb, 128), 1) + 128 * i == rid + k0, v[i], 0.0), axis=1, keepdims=True)
        sc = 1.0 / jnp.sqrt(dg)
        for i in tiles:
            v[i] = v[i] * sc
        linv[k0:k0 + nb, 0:128] = v[2]
        if 3 in v:
            linv[k0:k0 + nb, 128:256] = v[3]
        if k0 + nb < T:
            lo = 128 if k0 + nb >= 128 else 0
            lhs = jnp.concatenate([v[i] for i in left if 128 * i >= lo], axis=1)
            off = k0 + nb - lo
            for i in tiles:
                if 128 * (i + 1) > lo:
                    cols = slice(128 * i, 128 * i + 128)
                    upd = dot(lhs, v[i], ((0,), (0,)), HI)
                    g[k0 + nb:T, cols] = g[k0 + nb:T, cols] - upd[off:off + T - k0 - nb, :]

    return [start] + [functools.partial(step, b) for b in range(T // nb)]


def body(a_ref, w_ref, og_ref, or_ref,
         at, bnc, wg, rt, lhs, mxx, q, ug, *rest):
    pbuf, prx, sb, rlr, rb, fin, finp = (rest[NK * i:NK * (i + 1)] for i in range(7))
    (ah, ap, oh, pacc, g, linv, sx, sr, mx, mr, trx, try_, trz, trp, dw, send, recv, lsem) = rest[7 * NK:]
    t = lax.axis_index("task")
    x, y, z = (lax.axis_index(n) for n in ROW)
    p = y * 4 + z
    r = x * 16 + p

    def add(v, d):
        return lax.rem(v + (4 + d), 4)

    def dev(dt=0, dx=0, dy=0, dz=0):
        return (1 - t if dt else t, add(x, dx) if dx else x, add(y, dy) if dy else y, add(z, dz) if dz else z)

    net = Net(send, recv)
    ws = pl.multiple_of((r * 7 // 8 - r // 63) * 128, 128)
    kx = pl.multiple_of(x * KX, 128)
    hc = pl.multiple_of(t * HALF, 128)
    hp = pl.multiple_of((1 - t) * HALF, 128)
    loads = [(a_ref.at[0, :, pl.ds(ws, 256)], dw), (a_ref.at[0, :, 0:256], rt.at[y, z]), (w_ref.at[0], wg.at[y, z]),
             (a_ref.at[0, :, pl.ds(kx, KX)], at.at[x]), (a_ref.at[0, :, pl.ds(hc, HALF)], ah)]
    loads = [pltpu.make_async_copy(a, b, lsem.at[i]) for i, (a, b) in enumerate(loads)]
    l_dw, l_rt, l_w, l_at, l_ah = loads
    for c in loads:
        c.start()
    bar = pltpu.get_barrier_semaphore()
    peers = [dev(dt=1)] + [dev(**{a: d}) for a in ("dx", "dy", "dz") for d in (1, -1, 2)]
    for d in peers:
        pl.semaphore_signal(bar, inc=1, device_id=d, device_id_type=MESH)
    pl.semaphore_wait(bar, len(peers))

    def spread(buf, val, pos, axis):
        buf[pos] = jnp.broadcast_to(val, (8, 128))
        return [net.go(buf.at[pos], buf.at[pos], dev(**{axis: d})) for d in (1, -1, 2)]

    def total(buf, copies):
        for c in copies:
            c.wait_recv()
        return buf[0] + buf[1] + (buf[2] + buf[3])

    def gather(sl):
        def nb(h, stage, d):
            axis = ("dy", "dz")[(h + stage) % 2]
            return dev(**{axis: d})

        def ref(h, part, a, b):
            return sl(h, part, a, b) if h == 0 else sl(h, part, b, a)

        first, second = (y, z), (z, y)
        st = {}

        def ph1(h):
            s = ref(h, None, first[h], second[h])
            st[h, "p"] = net.go(s, s, nb(h, 0, 1))
            st[h, "m"] = net.go(s, s, nb(h, 0, -1))

        def ph2(h, k, a):
            s = ref(h, None, a, second[h])
            st[h, k, "p"] = net.go(s, s, nb(h, 1, 1))
            st[h, k, "m"] = net.go(s, s, nb(h, 1, -1))

        def fw1(h, side):
            d = -1 if side == "p" else 1
            st[h, side].wait_recv()
            s = ref(h, 0 if side == "p" else 1, add(first[h], d), second[h])
            st[h, "f" + side] = net.go(s, s, nb(h, 0, -d))

        def end1(h):
            st[h, "fp"].wait_recv()
            st[h, "fm"].wait_recv()

        def fw2(h, k, a, side):
            d = -1 if side == "p" else 1
            st[h, k, side].wait_recv()
            s = ref(h, 0 if side == "p" else 1, a, add(second[h], d))
            st[h, k, "f" + side] = net.go(s, s, nb(h, 1, -d))

        def end2(h, k):
            st[h, k, "fp"].wait_recv()
            st[h, k, "fm"].wait_recv()

        both = (0, 1)
        idx = {k: (lambda h, d=d: add(first[h], d) if d else first[h]) for k, d in ((0, 0), (1, -1), (2, 1), (3, 2))}

        def far(k):
            return [lambda h=h, side=side: fw2(h, k, idx[k](h), side) for h in both for side in "pm"]

        return dict(
            start=[lambda: [ph1(h) for h in both]],
            own=[lambda: [ph2(h, 0, first[h]) for h in both]],
            fw1=[lambda h=h, side=side: fw1(h, side) for side in "pm" for h in both],
            near=[lambda h=h, k=k: ph2(h, k, idx[k](h)) for k in (1, 2) for h in both],
            opp=[lambda h=h: (end1(h), ph2(h, 3, idx[3](h))) for h in both],
            f0=far(0), f1=far(1), f2=far(2), f3=far(3),
            end=[lambda: [end2(h, k) for k in range(4) for h in both]])

    def sl_rt(h, part, a, b):
        rows = slice(None) if part is None else pl.ds(56 * part, 56)
        return rt.at[a, b, rows, pl.ds(128 * h, 128)]

    def sl_w(k, h, part, a, b):
        lo, n = 1024 * h + sum(CHUNKS[:k]), CHUNKS[k]
        if part is not None:
            lo, n = lo + n // 2 * part, n // 2
        return wg.at[a, b, :, pl.ds(lo, n)]

    def sl_u(h, part, a, b):
        blk = slice(None) if part is None else part
        return ug.at[blk, a, b, :, pl.ds(128 * h, 128)]

    ev_r = gather(sl_rt)
    ev_w = [gather(functools.partial(sl_w, k)) for k in range(NK)]
    ev_u = gather(sl_u)

    def order(e, *names):
        return [f for n in names for f in e[n]]

    ev_r = order(ev_r, "start", "own", "fw1", "near", "f0", "opp", "f1", "f2", "f3", "end")

    def pump(ev, n=1):
        for _ in range(min(n, len(ev))):
            ev.pop(0)()

    l_dw.wait()
    tile = iota((B, 256), 1) == iota((B, 256), 0) + (r * B - ws)
    part = jnp.sum(jnp.where(tile, dw[...], 0.0), axis=1, keepdims=True)
    part = jnp.sum(part, axis=0, keepdims=True)
    cs = spread(trx, part, x, "dx")
    l_rt.wait()
    pump(ev_r, 2)

    def acol(d):
        return pl.ds(pl.multiple_of(add(x, d) * KX, 128), KX)

    n_early = len(net.all)
    xb = [net.go(a_ref.at[0, 0:56, acol(2)], bnc.at[0], dev(dx=1)),
          net.go(a_ref.at[0, 56:112, acol(2)], bnc.at[1], dev(dx=-1))]
    xd = [net.go(a_ref.at[0, :, acol(1)], at.at[x], dev(dx=1)),
          net.go(a_ref.at[0, :, acol(-1)], at.at[x], dev(dx=-1))]
    xp = net.go(a_ref.at[0, :, pl.ds(hp, HALF)], ap, dev(dt=1))
    xf = []
    l_w.wait()
    ev_w[0]["start"][0]()

    def relay0():
        xb[0].wait_recv()
        xf.append(net.go(bnc.at[0], at.at[add(x, -1), 0:56], dev(dx=1)))

    def relay1():
        xb[1].wait_recv()
        xf.append(net.go(bnc.at[1], at.at[add(x, 1), 56:112], dev(dx=-1)))

    ev_a = [relay0, relay1]

    old = []
    s = total(trx, cs)
    cs = spread(try_, s, y, "dy")
    a0 = len(net.all)
    pump(ev_r, 8)
    old += [c for c, _ in net.all[a0:]]
    ev_w[0]["own"][0]()
    s = total(try_, cs)
    cs = spread(trz, s, z, "dz")
    a0 = len(net.all)
    pump(ev_r, 6)
    old += [c for c, _ in net.all[a0:]]
    s = total(trz, cs)
    scale8 = float(H) / s
    trp[0] = scale8
    cp = net.go(trp.at[0], trp.at[1], dev(dt=1))
    scale = scale8[0:1, 0:1]
    for e in [ev_w[0]["fw1"], ev_w[0]["near"][:2], []]:
        for f in e:
            f()
        a0 = len(net.all)
        pump(ev_r, 4)
        old += [c for c, _ in net.all[a0:]]
    a0 = len(net.all)
    pump(ev_r, 99)
    old += [c for c, _ in net.all[a0:]]

    lane = iota((B, 256), 1)
    hit = lane == iota((B, 256), 0) + r * B
    mx[...] = jnp.where(lane < T, rt[y, z] * jnp.where(hit, scale, 0.9 * scale), 0.0)
    cm = net.go(mx, mr, dev(dt=1))
    for i in range(2):
        hit = lane == iota((B, 256), 0) + i * B
        sx[i] = jnp.where(lane < T, rt[0, i] * jnp.where(hit, scale, 0.9 * scale), 0.0)
    cS = net.go(sx, sr, dev(dt=1))
    cp.wait_recv()
    scale_p = trp[1][0:1, 0:1]
    cm.wait_recv()
    mxx[x] = mx[...] + mr[...]
    mine = pl.ds(pl.multiple_of(t * 56, 8), 56)
    cu = [net.go(mxx.at[x, mine], mxx.at[x, mine], dev(dx=d)) for d in (1, -1, 2)]
    pump(ev_a, 2)
    cS.wait_recv()

    net.retire(n_early)
    late = [c for c in net.all if any(c[0] is d for d in old)]
    net.all = late + [c for c in net.all if not any(c[0] is d for d in old)]
    net.retire(len(late))
    w0, w1 = ev_w
    ev = (w0["near"][2:] + w1["start"] + order(w0, "f0", "opp", "f1") + w1["own"] + w0["f2"] + w1["fw1"]
          + order(w0, "f3", "end") + order(w1, "opp", "near", "f0"))

    def until(e):
        while any(v is e["end"][0] for v in ev):
            pump(ev)

    for f in chol_steps(g, linv, lambda i: sx[i] + sr[i]):
        pl.when(x == 0)(f)
        pump(ev, 3)

    regions = [linv.at[pl.ds(pl.multiple_of(B * t, 8), B), 0:128],
               linv.at[pl.ds(pl.multiple_of(128 + 48 * t, 8), 48), 128:256]]
    lc, lp = [], []
    for v in regions:
        first = net.n
        lc.append([net.copy(v, v, dev(dx=d), track=False, like=first) for d in (1, 2, -1)])
    for v in regions:
        lp.append(net.copy(v, v, dev(dt=1), track=False))

    @pl.when(x == 0)
    def _():
        linv[0:128, 128:256] = jnp.zeros((128, 128), F32)
        for cc in lc:
            for c in cc:
                c.start()

    @pl.when(x > 0)
    def _():
        linv[T:256, :] = jnp.zeros((256 - T, 256), F32)
        linv[0:128, 128:256] = jnp.zeros((128, 128), F32)

    v = rt[...].reshape(KX, 256)
    hit = iota((KX, 256), 0) + x * KX == iota((KX, 256), 1)
    v = jnp.where(iota((KX, 256), 1) < T, v * jnp.where(hit, 1.0, 0.9), 0.0)
    v = v.T

    def put(name, v):
        o, m, _ = GROUPS[name]
        lhs[o:o + m, :], lhs[o + m:o + 2 * m, :] = split(v)

    put("z", v)
    pump(ev, 3)

    def tile_in(name, d):
        v = at[add(x, d)]
        if d == 0:
            hit = iota((B, KX), 1) == iota((B, KX), 0) + p * B
            v = v * jnp.where(hit, 1.0, 0.9)
        else:
            v = v * 0.9
        put(name, v)

    l_at.wait()
    tile_in("own", 0)
    xd[1].wait_recv()
    tile_in("p1", 1)
    xd[0].wait_recv()
    tile_in("m1", -1)

    def rows_of(k, j, *names):
        n = CHUNKS[k]
        lo = pl.multiple_of((t if j else 1 - t) * 1024 + sum(CHUNKS[:k]), 256)
        wcol = wg[:, :, :, pl.ds(lo, n)].reshape(KX, n)
        first = GROUPS[names[0]][0]
        last, m, _ = GROUPS[names[-1]]
        acc = dot(lhs[first:last + 2 * m], wcol)
        for name in names:
            o, m, to = GROUPS[name]
            o = o - first
            pacc[j, to:to + m, 0:n] = acc[o:o + m] + acc[o + m:o + 2 * m]

    until(w0)
    early = [(j, names) for j in range(2) for names in (("z",), ("p1", "m1", "own"))]
    rows_of(0, 0, *early[0][1])
    pump(ev, 2)
    for c in cu:
        c.wait_recv()
    cv = []
    for d in (1, -1, 2):
        v = mxx.at[add(x, d), mine]
        cv.append(net.go(v, v, dev(dt=1)))

    @pl.when(x > 0)
    def _():
        for cc in lc:
            cc[0].wait_recv()
        for c in lp:
            c.start()
        for c in lp:
            c.wait_recv()

    pump(ev, 2)
    for c in cv:
        c.wait_recv()

    lin = split(linv[...])
    ut = dot3(split(mxx[...].reshape(448, 256)), lin, ((1,), (1,)))
    for i in range(4):
        q[i] = ut[B * i:B * (i + 1)]
    for i in range(2):
        ug[i, y, z] = q[2 * t + i]
    ev += (order(w1, "f3", "f1", "f2") + order(ev_u, "start", "own") + w1["end"]
           + order(ev_u, "fw1", "near", "opp", "f0", "f1", "f2", "f3", "end"))
    ident = iota((B, 256), 1) - iota((B, 256), 0)

    def rows_q(d):
        xx = add(x, d)
        top = (xx * 16 + p < 2).astype(F32)
        sel = jnp.where(ident == p * B, -1.0, 0.0)
        return q[xx] * (1.0 - top) + sel * top, 1.0 - top

    qs = [rows_q(d) for d in (0, 1, -1, 2)]
    keep = qs[0][1]
    qc = split(qs[0][0])
    qg = split(jnp.concatenate([v for v, _ in qs], axis=0))

    ys = {}

    def solve(k, j):
        ys[k, j] = split(dot3(lin, split(pacc[j, 0:256, 0:CHUNKS[k]])))

    def correct(k, j, lo, hi):
        n = CHUNKS[k]
        cor = dot3([v[B * lo:B * hi] for v in qg], ys[k, j])
        for i in range(lo, hi):
            pc = pacc[j, 256 + B * i:256 + B * (i + 1), 0:n] * qs[i][1]
            pbuf[k][j, i] = (pc - cor[B * (i - lo):B * (i + 1 - lo)]) * scale

    rs = {}

    def pair_send(k, lo, hi):
        rs[k, "d", lo] = net.go(pbuf[k].at[0, lo:hi], prx[k].at[lo:hi], dev(dt=1))

    def pair_sum(k, lo, hi):
        rs[k, "d", lo].wait_recv()
        n = CHUNKS[k] // 2
        for i in range(lo, hi):
            for j in range(2):
                cols = slice(n * j, n * j + n)
                sb[k][i, j] = pbuf[k][1, i, :, cols] + prx[k][i, :, cols]

    def rs0(k):
        rs[k, 0] = net.go(sb[k].at[3, 0], rlr[k].at[0], dev(dx=1))
        rs[k, 1] = net.go(sb[k].at[3, 1], rlr[k].at[1], dev(dx=-1))

    def rs1(k):
        rs[k, 0].wait_recv()
        sb[k][1, 0] = sb[k][1, 0] + rlr[k][0]
        rs[k, 2] = net.go(sb[k].at[1], rb[k].at[0], dev(dx=1))
        rs[k, 1].wait_recv()
        sb[k][2, 1] = sb[k][2, 1] + rlr[k][1]
        rs[k, 3] = net.go(sb[k].at[2], rb[k].at[1], dev(dx=-1))

    def rs2(k):
        rs[k, 2].wait_recv()
        rs[k, 3].wait_recv()
        fin[k][...] = sb[k][0] + (rb[k][0] + rb[k][1])
        rs[k, 4] = net.go(fin[k], finp[k], dev(dt=1))

    def rs3(k):
        rs[k, 4].wait_recv()
        n = CHUNKS[k] // 2
        for j in range(2):
            lo = sum(CHUNKS[:k]) + n * j
            or_ref[:, pl.ds(pl.multiple_of(t * 1024 + lo, 128), n)] = fin[k][j]
            or_ref[:, pl.ds(pl.multiple_of((1 - t) * 1024 + lo, 128), n)] = finp[k][j]

    for j, names in early[1:]:
        rows_of(0, j, *names)
        pump(ev, 2)
    for c in xf:
        c.wait_recv()
    tile_in("opp", 2)
    for j in range(2):
        rows_of(0, j, "opp")
    for j in range(2):
        solve(0, j)
        correct(0, j, 0, 4)
        if j == 0:
            pair_send(0, 0, 4)
        pump(ev, 2)
    pair_sum(0, 0, 4)
    rs0(0)
    l_ah.wait()
    xp.wait_recv()
    hit = iota((B, HALF), 1) == iota((B, HALF), 0) + (r * B - t * HALF)
    m = ah[...] * (scale * keep) + ap[...] * (scale_p * keep)
    oh[...] = m * jnp.where(hit, 1.0, 0.9)
    pump(ev, 4)
    until(w1)
    for j in range(2):
        rows_of(1, j, "opp", "z")
        solve(1, j)
        correct(1, j, 3, 4)
        if j == 0:
            pair_send(1, 3, 4)
            rs1(0)
        pump(ev, 3)
    pair_sum(1, 3, 4)
    rs0(1)
    for j in range(2):
        rows_of(1, j, "p1", "m1")
        correct(1, j, 1, 3)
        if j == 0:
            pair_send(1, 1, 3)
        pump(ev, 4)
    pair_sum(1, 1, 3)
    rs1(1)
    for j in range(2):
        rows_of(1, j, "own")
        correct(1, j, 0, 1)
        if j == 0:
            pair_send(1, 0, 1)
        pump(ev, 5)
    pair_sum(1, 0, 1)
    rs2(0)
    pump(ev, 3)
    rs3(0)
    pump(ev, 99)
    out = []
    for i in range(2):
        for c in range(7):
            cols = slice((i * 7 + c) * 256, (i * 7 + c + 1) * 256)
            u = split(ug[i].reshape(KX, 256)[c * 256:(c + 1) * 256])
            oh[:, cols] = oh[:, cols] - dot3(qc, u, ((1,), (1,)))
        src = oh.at[:, i * KX:(i + 1) * KX]
        dst = og_ref.at[:, pl.ds(pl.multiple_of(t * HALF + i * KX, 128), KX)]
        co = pltpu.make_async_copy(src, dst, lsem.at[5 + i])
        co.start()
        out.append((co, net.go(src, dst, dev(dt=1))))
        if i == 0:
            rs2(1)
    rs3(1)
    for co, cg in out:
        co.wait()
        cg.wait_recv()
    net.retire(len(net.all))

    @pl.when(x == 0)
    def _():
        for cc in lc:
            for c in cc:
                c.wait_send()

    @pl.when(x > 0)
    def _():
        for c in lp:
            c.wait_send()

    assert net.n <= NCOPY and net.sends <= NSEND, (net.n, net.sends)


def per_device(grams, weights):
    V = pltpu.VMEM
    scratch = [
        V((4, B, KX), F32), V((2, 56, KX), F32), V((4, 4, B, DC), BF16), V((4, 4, B, 256), F32),
        V((1408, KX), BF16), V((4, B, 256), F32), V((4, B, 256), F32), V((2, 4, 4, B, 256), F32),
        *[V((2, 4, B, n), F32) for n in CHUNKS], *[V((4, B, n), F32) for n in CHUNKS],
        *[V((4, 2, B, n // 2), F32) for n in CHUNKS], *[V((2, B, n // 2), F32) for n in CHUNKS],
        *[V((2, 2, B, n // 2), F32) for n in CHUNKS], *[V((2, B, n // 2), F32) for n in CHUNKS],
        *[V((2, B, n // 2), F32) for n in CHUNKS],
        V((B, HALF), F32), V((B, HALF), F32), V((B, HALF), F32), V((2, 704, 512), F32), V((T, 512), F32), V((256, 256), F32),
        V((2, B, 256), F32), V((2, B, 256), F32), V((B, 256), F32), V((B, 256), F32),
        V((4, 8, 128), F32), V((4, 8, 128), F32), V((4, 8, 128), F32), V((2, 8, 128), F32), V((B, 256), F32),
        pltpu.SemaphoreType.DMA((NSEND,)), pltpu.SemaphoreType.DMA((NCOPY,)), pltpu.SemaphoreType.DMA((8,)),
    ]
    return pl.pallas_call(
        body,
        out_shape=(pltpu.VMEM((B, H), F32), pltpu.VMEM((B, DC), F32)),
        in_specs=[pl.BlockSpec(memory_space=pl.ANY)] * 2,
        out_specs=(pl.BlockSpec(memory_space=pltpu.VMEM), pl.BlockSpec(memory_space=pltpu.VMEM)),
        scratch_shapes=scratch,
        compiler_params=pltpu.CompilerParams(
            collective_id=0, has_side_effects=True, vmem_limit_bytes=57 * 1024 * 1024),
    )(grams, weights)


def solution(mesh):
    torus = Mesh(mesh.devices.reshape(mesh.shape["task"], 4, 4, 4), ("task",) + ROW)
    return jax.shard_map(
        per_device, mesh=torus, in_specs=(P("task", ROW, None), P("task", ROW, None)),
        out_specs=(P(ROW, None), P(ROW, None)), check_vma=False)
```

```python
import functools

import jax
import jax.numpy as jnp
from jax import lax
from jax.experimental import pallas as pl
from jax.experimental.pallas import tpu as pltpu
from jax.sharding import Mesh
from jax.sharding import PartitionSpec as P

ROW = ("row_0", "row_1", "row_2")
F32 = jnp.float32
BF16 = jnp.bfloat16
B = 112
T = 224
H = 7168
DC = 2048
KX = 1792
HALF = 3584
MESH = pl.DeviceIdType.MESH
HI = lax.Precision.HIGHEST
NCOPY = 216
NSEND = 200
CHUNKS = (512, 512)
NK = len(CHUNKS)


class Net:
    def __init__(self, send, recv):
        self.send, self.recv, self.n, self.all, self.sends, self.free = send, recv, 0, [], 0, []

    def copy(self, src, dst, dev, track=True, like=None):
        i = self.n
        self.n += 1
        k = i if like is None else like
        if self.free:
            j = self.free.pop()
        else:
            j = self.sends
            self.sends += 1
        c = pltpu.make_async_remote_copy(
            src_ref=src, dst_ref=dst, send_sem=self.send.at[j], recv_sem=self.recv.at[k],
            device_id=dev, device_id_type=MESH)
        if track:
            self.all.append((c, j))
        return c

    def retire(self, n):
        for c, j in self.all[:n]:
            c.wait_send()
            self.free.append(j)
        del self.all[:n]

    def go(self, src, dst, dev):
        c = self.copy(src, dst, dev)
        c.start()
        return c


def iota(shape, dim):
    return lax.broadcasted_iota(jnp.int32, shape, dim)


def dot(a, b, dims=((1,), (0,)), precision=None):
    return lax.dot_general(a, b, (dims, ((), ())), precision=precision, preferred_element_type=F32)


def split(v):
    hi = v.astype(BF16)
    return hi, (v - hi.astype(F32)).astype(BF16)


def dot3(a, b, dims=((1,), (0,))):
    return dot(a[0], b[0], dims) + (dot(a[0], b[1], dims) + dot(a[1], b[0], dims))


GROUPS = dict(opp=(0, B, 592), z=(224, 256, 0), p1=(736, B, 368), m1=(960, B, 480), own=(1184, B, 256))


def chol_steps(g, linv, corner):
    nb = 32

    def start():
        linv[T:256, 0:128] = jnp.zeros((256 - T, 128), F32)
        linv[T:256, 128:256] = jnp.zeros((256 - T, 128), F32)
        for i in range(2):
            g[B * i:B * (i + 1), 0:256] = corner(i)
        g[:, 256:512] = jnp.where(iota((T, 256), 0) == iota((T, 256), 1), 1.0, 0.0)

    def step(b):
        rid = iota((nb, 128), 0)
        k0 = nb * b
        left = [i for i in (0, 1) if 128 * (i + 1) > k0]
        tiles = left + [2] + ([3] if k0 + nb > 128 else [])
        v = {i: g[k0:k0 + nb, 128 * i:128 * i + 128] for i in tiles}

        def column(k):
            i = k // 128
            return jnp.broadcast_to(v[i][:, k % 128:k % 128 + 1], (nb, 128))

        for j in range(0, nb, 2):
            c0, c1 = column(k0 + j), column(k0 + j + 1)
            d00, d01, d11 = c0[j:j + 1], c1[j:j + 1], c1[j + 1:j + 2]
            inv = 1.0 / (d00 * d11 - d01 * d01)
            f0 = jnp.where(rid > j + 1, (d11 * inv) * c0 - (d01 * inv) * c1, 0.0)
            f1 = jnp.where(rid > j + 1, (d00 * inv) * c1 - (d01 * inv) * c0, 0.0)
            f0 = jnp.where(rid == j + 1, d01 / d00, f0)
            for i in tiles:
                v[i] = v[i] - f0 * v[i][j:j + 1, :] - f1 * v[i][j + 1:j + 2, :]
        dg = 0.0
        for i in left:
            dg = dg + jnp.sum(jnp.where(iota((nb, 128), 1) + 128 * i == rid + k0, v[i], 0.0), axis=1, keepdims=True)
        sc = 1.0 / jnp.sqrt(dg)
        for i in tiles:
            v[i] = v[i] * sc
        linv[k0:k0 + nb, 0:128] = v[2]
        if 3 in v:
            linv[k0:k0 + nb, 128:256] = v[3]
        if k0 + nb < T:
            lo = 128 if k0 + nb >= 128 else 0
            lhs = jnp.concatenate([v[i] for i in left if 128 * i >= lo], axis=1)
            off = k0 + nb - lo
            for i in tiles:
                if 128 * (i + 1) > lo:
                    cols = slice(128 * i, 128 * i + 128)
                    upd = dot(lhs, v[i], ((0,), (0,)), HI)
                    g[k0 + nb:T, cols] = g[k0 + nb:T, cols] - upd[off:off + T - k0 - nb, :]

    return [start] + [functools.partial(step, b) for b in range(T // nb)]


def body(a_ref, w_ref, og_ref, or_ref,
         at, bnc, wg, rt, lhs, mxx, q, ug, *rest):
    pbuf, prx, sb, rlr, rb, fin, finp = (rest[NK * i:NK * (i + 1)] for i in range(7))
    (ah, ap, oh, pacc, g, linv, sx, sr, mx, mr, trx, try_, trz, trp, dw, send, recv, lsem) = rest[7 * NK:]
    t = lax.axis_index("task")
    x, y, z = (lax.axis_index(n) for n in ROW)
    p = y * 4 + z
    r = x * 16 + p

    def add(v, d):
        return lax.rem(v + (4 + d), 4)

    def dev(dt=0, dx=0, dy=0, dz=0):
        return (1 - t if dt else t, add(x, dx) if dx else x, add(y, dy) if dy else y, add(z, dz) if dz else z)

    net = Net(send, recv)
    ws = pl.multiple_of((r * 7 // 8 - r // 63) * 128, 128)
    kx = pl.multiple_of(x * KX, 128)
    hc = pl.multiple_of(t * HALF, 128)
    hp = pl.multiple_of((1 - t) * HALF, 128)
    loads = [(a_ref.at[0, :, pl.ds(ws, 256)], dw), (a_ref.at[0, :, 0:256], rt.at[y, z]), (w_ref.at[0], wg.at[y, z]),
             (a_ref.at[0, :, pl.ds(kx, KX)], at.at[x]), (a_ref.at[0, :, pl.ds(hc, HALF)], ah)]
    loads = [pltpu.make_async_copy(a, b, lsem.at[i]) for i, (a, b) in enumerate(loads)]
    l_dw, l_rt, l_w, l_at, l_ah = loads
    for c in loads:
        c.start()
    bar = pltpu.get_barrier_semaphore()
    peers = [dev(dt=1)] + [dev(**{a: d}) for a in ("dx", "dy", "dz") for d in (1, -1, 2)]
    for d in peers:
        pl.semaphore_signal(bar, inc=1, device_id=d, device_id_type=MESH)
    pl.semaphore_wait(bar, len(peers))

    def spread(buf, val, pos, axis):
        buf[pos] = jnp.broadcast_to(val, (8, 128))
        return [net.go(buf.at[pos], buf.at[pos], dev(**{axis: d})) for d in (1, -1, 2)]

    def total(buf, copies):
        for c in copies:
            c.wait_recv()
        return buf[0] + buf[1] + (buf[2] + buf[3])

    def gather(sl):
        def nb(h, stage, d):
            axis = ("dy", "dz")[(h + stage) % 2]
            return dev(**{axis: d})

        def ref(h, part, a, b):
            return sl(h, part, a, b) if h == 0 else sl(h, part, b, a)

        first, second = (y, z), (z, y)
        st = {}

        def ph1(h):
            s = ref(h, None, first[h], second[h])
            st[h, "p"] = net.go(s, s, nb(h, 0, 1))
            st[h, "m"] = net.go(s, s, nb(h, 0, -1))

        def ph2(h, k, a):
            s = ref(h, None, a, second[h])
            st[h, k, "p"] = net.go(s, s, nb(h, 1, 1))
            st[h, k, "m"] = net.go(s, s, nb(h, 1, -1))

        def fw1(h, side):
            d = -1 if side == "p" else 1
            st[h, side].wait_recv()
            s = ref(h, 0 if side == "p" else 1, add(first[h], d), second[h])
            st[h, "f" + side] = net.go(s, s, nb(h, 0, -d))

        def end1(h):
            st[h, "fp"].wait_recv()
            st[h, "fm"].wait_recv()

        def fw2(h, k, a, side):
            d = -1 if side == "p" else 1
            st[h, k, side].wait_recv()
            s = ref(h, 0 if side == "p" else 1, a, add(second[h], d))
            st[h, k, "f" + side] = net.go(s, s, nb(h, 1, -d))

        def end2(h, k):
            st[h, k, "fp"].wait_recv()
            st[h, k, "fm"].wait_recv()

        both = (0, 1)
        idx = {k: (lambda h, d=d: add(first[h], d) if d else first[h]) for k, d in ((0, 0), (1, -1), (2, 1), (3, 2))}

        def far(k):
            return [lambda h=h, side=side: fw2(h, k, idx[k](h), side) for h in both for side in "pm"]

        return dict(
            start=[lambda: [ph1(h) for h in both]],
            own=[lambda: [ph2(h, 0, first[h]) for h in both]],
            fw1=[lambda h=h, side=side: fw1(h, side) for side in "pm" for h in both],
            near=[lambda h=h, k=k: ph2(h, k, idx[k](h)) for k in (1, 2) for h in both],
            opp=[lambda h=h: (end1(h), ph2(h, 3, idx[3](h))) for h in both],
            f0=far(0), f1=far(1), f2=far(2), f3=far(3),
            end=[lambda: [end2(h, k) for k in range(4) for h in both]])

    def sl_rt(h, part, a, b):
        rows = slice(None) if part is None else pl.ds(56 * part, 56)
        return rt.at[a, b, rows, pl.ds(128 * h, 128)]

    def sl_w(k, h, part, a, b):
        lo, n = 1024 * h + sum(CHUNKS[:k]), CHUNKS[k]
        if part is not None:
            lo, n = lo + n // 2 * part, n // 2
        return wg.at[a, b, :, pl.ds(lo, n)]

    def sl_u(h, part, a, b):
        blk = slice(None) if part is None else part
        return ug.at[blk, a, b, :, pl.ds(128 * h, 128)]

    ev_r = gather(sl_rt)
    ev_w = [gather(functools.partial(sl_w, k)) for k in range(NK)]
    ev_u = gather(sl_u)

    def order(e, *names):
        return [f for n in names for f in e[n]]

    ev_r = order(ev_r, "start", "own", "fw1", "near", "f0", "opp", "f1", "f2", "f3", "end")

    def pump(ev, n=1):
        for _ in range(min(n, len(ev))):
            ev.pop(0)()

    l_dw.wait()
    tile = iota((B, 256), 1) == iota((B, 256), 0) + (r * B - ws)
    part = jnp.sum(jnp.where(tile, dw[...], 0.0), axis=1, keepdims=True)
    part = jnp.sum(part, axis=0, keepdims=True)
    cs = spread(trx, part, x, "dx")
    l_rt.wait()
    pump(ev_r, 2)

    def acol(d):
        return pl.ds(pl.multiple_of(add(x, d) * KX, 128), KX)

    n_early = len(net.all)
    xb = [net.go(a_ref.at[0, 0:56, acol(2)], bnc.at[0], dev(dx=1)),
          net.go(a_ref.at[0, 56:112, acol(2)], bnc.at[1], dev(dx=-1))]
    xd = [net.go(a_ref.at[0, :, acol(1)], at.at[x], dev(dx=1)),
          net.go(a_ref.at[0, :, acol(-1)], at.at[x], dev(dx=-1))]
    xp = net.go(a_ref.at[0, :, pl.ds(hp, HALF)], ap, dev(dt=1))
    xf = []
    l_w.wait()
    ev_w[0]["start"][0]()

    def relay0():
        xb[0].wait_recv()
        xf.append(net.go(bnc.at[0], at.at[add(x, -1), 0:56], dev(dx=1)))

    def relay1():
        xb[1].wait_recv()
        xf.append(net.go(bnc.at[1], at.at[add(x, 1), 56:112], dev(dx=-1)))

    ev_a = [relay0, relay1]

    old = []
    s = total(trx, cs)
    cs = spread(try_, s, y, "dy")
    a0 = len(net.all)
    pump(ev_r, 8)
    old += [c for c, _ in net.all[a0:]]
    ev_w[0]["own"][0]()
    s = total(try_, cs)
    cs = spread(trz, s, z, "dz")
    a0 = len(net.all)
    pump(ev_r, 6)
    old += [c for c, _ in net.all[a0:]]
    s = total(trz, cs)
    scale8 = float(H) / s
    trp[0] = scale8
    cp = net.go(trp.at[0], trp.at[1], dev(dt=1))
    scale = scale8[0:1, 0:1]
    for e in [ev_w[0]["fw1"], ev_w[0]["near"][:2], []]:
        for f in e:
            f()
        a0 = len(net.all)
        pump(ev_r, 4)
        old += [c for c, _ in net.all[a0:]]
    a0 = len(net.all)
    pump(ev_r, 99)
    old += [c for c, _ in net.all[a0:]]

    lane = iota((B, 256), 1)
    hit = lane == iota((B, 256), 0) + r * B
    mx[...] = jnp.where(lane < T, rt[y, z] * jnp.where(hit, scale, 0.9 * scale), 0.0)
    cm = net.go(mx, mr, dev(dt=1))
    for i in range(2):
        hit = lane == iota((B, 256), 0) + i * B
        sx[i] = jnp.where(lane < T, rt[0, i] * jnp.where(hit, scale, 0.9 * scale), 0.0)
    cS = net.go(sx, sr, dev(dt=1))
    cp.wait_recv()
    scale_p = trp[1][0:1, 0:1]
    cm.wait_recv()
    mxx[x] = mx[...] + mr[...]
    mine = pl.ds(pl.multiple_of(t * 56, 8), 56)
    cu = [net.go(mxx.at[x, mine], mxx.at[x, mine], dev(dx=d)) for d in (1, -1, 2)]
    pump(ev_a, 2)
    cS.wait_recv()

    net.retire(n_early)
    late = [c for c in net.all if any(c[0] is d for d in old)]
    net.all = late + [c for c in net.all if not any(c[0] is d for d in old)]
    net.retire(len(late))
    w0, w1 = ev_w
    ev = (w0["near"][2:] + w1["start"] + order(w0, "f0", "opp", "f1") + w1["own"] + w0["f2"] + w1["fw1"]
          + order(w0, "f3", "end") + order(w1, "opp", "near", "f0"))

    def until(e):
        while any(v is e["end"][0] for v in ev):
            pump(ev)

    for f in chol_steps(g, linv, lambda i: sx[i] + sr[i]):
        pl.when(x == 0)(f)
        pump(ev, 3)

    regions = [linv.at[pl.ds(pl.multiple_of(B * t, 8), B), 0:128],
               linv.at[pl.ds(pl.multiple_of(128 + 48 * t, 8), 48), 128:256]]
    lc, lp = [], []
    for v in regions:
        first = net.n
        lc.append([net.copy(v, v, dev(dx=d), track=False, like=first) for d in (1, 2, -1)])
    for v in regions:
        lp.append(net.copy(v, v, dev(dt=1), track=False))

    @pl.when(x == 0)
    def _():
        linv[0:128, 128:256] = jnp.zeros((128, 128), F32)
        for cc in lc:
            for c in cc:
                c.start()

    @pl.when(x > 0)
    def _():
        linv[T:256, :] = jnp.zeros((256 - T, 256), F32)
        linv[0:128, 128:256] = jnp.zeros((128, 128), F32)

    v = rt[...].reshape(KX, 256)
    hit = iota((KX, 256), 0) + x * KX == iota((KX, 256), 1)
    v = jnp.where(iota((KX, 256), 1) < T, v * jnp.where(hit, 1.0, 0.9), 0.0)
    v = v.T

    def put(name, v):
        o, m, _ = GROUPS[name]
        lhs[o:o + m, :], lhs[o + m:o + 2 * m, :] = split(v)

    put("z", v)
    pump(ev, 3)

    def tile_in(name, d):
        v = at[add(x, d)]
        if d == 0:
            hit = iota((B, KX), 1) == iota((B, KX), 0) + p * B
            v = v * jnp.where(hit, 1.0, 0.9)
        else:
            v = v * 0.9
        put(name, v)

    l_at.wait()
    tile_in("own", 0)
    xd[1].wait_recv()
    tile_in("p1", 1)
    xd[0].wait_recv()
    tile_in("m1", -1)

    def rows_of(k, j, *names):
        n = CHUNKS[k]
        lo = pl.multiple_of((t if j else 1 - t) * 1024 + sum(CHUNKS[:k]), 256)
        wcol = wg[:, :, :, pl.ds(lo, n)].reshape(KX, n)
        first = GROUPS[names[0]][0]
        last, m, _ = GROUPS[names[-1]]
        acc = dot(lhs[first:last + 2 * m], wcol)
        for name in names:
            o, m, to = GROUPS[name]
            o = o - first
            pacc[j, to:to + m, 0:n] = acc[o:o + m] + acc[o + m:o + 2 * m]

    until(w0)
    early = [(j, names) for j in range(2) for names in (("z",), ("p1", "m1", "own"))]
    rows_of(0, 0, *early[0][1])
    pump(ev, 6)
    for c in cu:
        c.wait_recv()
    cv = []
    for d in (1, -1, 2):
        v = mxx.at[add(x, d), mine]
        cv.append(net.go(v, v, dev(dt=1)))

    @pl.when(x > 0)
    def _():
        for cc in lc:
            cc[0].wait_recv()
        for c in lp:
            c.start()
        for c in lp:
            c.wait_recv()

    pump(ev, 2)
    for c in cv:
        c.wait_recv()

    lin = split(linv[...])
    ut = dot3(split(mxx[...].reshape(448, 256)), lin, ((1,), (1,)))
    for i in range(4):
        q[i] = ut[B * i:B * (i + 1)]
    for i in range(2):
        ug[i, y, z] = q[2 * t + i]
    ev += (order(w1, "f3", "f1", "f2") + order(ev_u, "start", "own") + w1["end"]
           + order(ev_u, "fw1", "near", "opp", "f0", "f1", "f2", "f3", "end"))
    ident = iota((B, 256), 1) - iota((B, 256), 0)

    def rows_q(d):
        xx = add(x, d)
        top = (xx * 16 + p < 2).astype(F32)
        sel = jnp.where(ident == p * B, -1.0, 0.0)
        return q[xx] * (1.0 - top) + sel * top, 1.0 - top

    qs = [rows_q(d) for d in (0, 1, -1, 2)]
    keep = qs[0][1]
    qc = split(qs[0][0])
    qg = split(jnp.concatenate([v for v, _ in qs], axis=0))

    ys = {}

    def solve(k, j):
        ys[k, j] = split(dot3(lin, split(pacc[j, 0:256, 0:CHUNKS[k]])))

    def correct(k, j, lo, hi):
        n = CHUNKS[k]
        cor = dot3([v[B * lo:B * hi] for v in qg], ys[k, j])
        for i in range(lo, hi):
            pc = pacc[j, 256 + B * i:256 + B * (i + 1), 0:n] * qs[i][1]
            pbuf[k][j, i] = (pc - cor[B * (i - lo):B * (i + 1 - lo)]) * scale

    rs = {}

    def pair_send(k, lo, hi):
        rs[k, "d", lo] = net.go(pbuf[k].at[0, lo:hi], prx[k].at[lo:hi], dev(dt=1))

    def pair_sum(k, lo, hi):
        rs[k, "d", lo].wait_recv()
        n = CHUNKS[k] // 2
        for i in range(lo, hi):
            for j in range(2):
                cols = slice(n * j, n * j + n)
                sb[k][i, j] = pbuf[k][1, i, :, cols] + prx[k][i, :, cols]

    def rs0(k):
        rs[k, 0] = net.go(sb[k].at[3, 0], rlr[k].at[0], dev(dx=1))
        rs[k, 1] = net.go(sb[k].at[3, 1], rlr[k].at[1], dev(dx=-1))

    def rs1(k):
        rs[k, 0].wait_recv()
        sb[k][1, 0] = sb[k][1, 0] + rlr[k][0]
        rs[k, 2] = net.go(sb[k].at[1], rb[k].at[0], dev(dx=1))
        rs[k, 1].wait_recv()
        sb[k][2, 1] = sb[k][2, 1] + rlr[k][1]
        rs[k, 3] = net.go(sb[k].at[2], rb[k].at[1], dev(dx=-1))

    def rs2(k):
        rs[k, 2].wait_recv()
        rs[k, 3].wait_recv()
        fin[k][...] = sb[k][0] + (rb[k][0] + rb[k][1])
        rs[k, 4] = net.go(fin[k], finp[k], dev(dt=1))

    def rs3(k):
        rs[k, 4].wait_recv()
        n = CHUNKS[k] // 2
        for j in range(2):
            lo = sum(CHUNKS[:k]) + n * j
            or_ref[:, pl.ds(pl.multiple_of(t * 1024 + lo, 128), n)] = fin[k][j]
            or_ref[:, pl.ds(pl.multiple_of((1 - t) * 1024 + lo, 128), n)] = finp[k][j]

    for j, names in early[1:]:
        rows_of(0, j, *names)
        pump(ev, 2)
    for c in xf:
        c.wait_recv()
    tile_in("opp", 2)
    for j in range(2):
        rows_of(0, j, "opp")
    for j in range(2):
        solve(0, j)
        correct(0, j, 0, 4)
        if j == 0:
            pair_send(0, 0, 4)
        pump(ev, 2)
    pair_sum(0, 0, 4)
    rs0(0)
    l_ah.wait()
    xp.wait_recv()
    hit = iota((B, HALF), 1) == iota((B, HALF), 0) + (r * B - t * HALF)
    m = ah[...] * (scale * keep) + ap[...] * (scale_p * keep)
    oh[...] = m * jnp.where(hit, 1.0, 0.9)
    pump(ev, 4)
    until(w1)
    for j in range(2):
        rows_of(1, j, "opp", "z")
        solve(1, j)
        correct(1, j, 3, 4)
        if j == 0:
            pair_send(1, 3, 4)
            rs1(0)
        pump(ev, 3)
    pair_sum(1, 3, 4)
    rs0(1)
    for j in range(2):
        rows_of(1, j, "p1", "m1")
        correct(1, j, 1, 3)
        if j == 0:
            pair_send(1, 1, 3)
        pump(ev, 4)
    pair_sum(1, 1, 3)
    rs1(1)
    for j in range(2):
        rows_of(1, j, "own")
        correct(1, j, 0, 1)
        if j == 0:
            pair_send(1, 0, 1)
        pump(ev, 5)
    pair_sum(1, 0, 1)
    rs2(0)
    pump(ev, 3)
    rs3(0)
    pump(ev, 99)
    out = []
    q2 = jnp.concatenate(qc, axis=0)
    for i in range(2):
        for c in range(7):
            cols = slice((i * 7 + c) * 256, (i * 7 + c + 1) * 256)
            u = split(ug[i].reshape(KX, 256)[c * 256:(c + 1) * 256])
            d = dot(q2, u[0], ((1,), (1,)))
            oh[:, cols] = oh[:, cols] - (d[0:B] + d[B:2 * B]) - dot(qc[0], u[1], ((1,), (1,)))
        src = oh.at[:, i * KX:(i + 1) * KX]
        dst = og_ref.at[:, pl.ds(pl.multiple_of(t * HALF + i * KX, 128), KX)]
        co = pltpu.make_async_copy(src, dst, lsem.at[5 + i])
        co.start()
        out.append((co, net.go(src, dst, dev(dt=1))))
        if i == 0:
            rs2(1)
    rs3(1)
    for co, cg in out:
        co.wait()
        cg.wait_recv()
    net.retire(len(net.all))

    @pl.when(x == 0)
    def _():
        for cc in lc:
            for c in cc:
                c.wait_send()

    @pl.when(x > 0)
    def _():
        for c in lp:
            c.wait_send()

    assert net.n <= NCOPY and net.sends <= NSEND, (net.n, net.sends)


def per_device(grams, weights):
    V = pltpu.VMEM
    scratch = [
        V((4, B, KX), F32), V((2, 56, KX), F32), V((4, 4, B, DC), BF16), V((4, 4, B, 256), F32),
        V((1408, KX), BF16), V((4, B, 256), F32), V((4, B, 256), F32), V((2, 4, 4, B, 256), F32),
        *[V((2, 4, B, n), F32) for n in CHUNKS], *[V((4, B, n), F32) for n in CHUNKS],
        *[V((4, 2, B, n // 2), F32) for n in CHUNKS], *[V((2, B, n // 2), F32) for n in CHUNKS],
        *[V((2, 2, B, n // 2), F32) for n in CHUNKS], *[V((2, B, n // 2), F32) for n in CHUNKS],
        *[V((2, B, n // 2), F32) for n in CHUNKS],
        V((B, HALF), F32), V((B, HALF), F32), V((B, HALF), F32), V((2, 704, 512), F32), V((T, 512), F32), V((256, 256), F32),
        V((2, B, 256), F32), V((2, B, 256), F32), V((B, 256), F32), V((B, 256), F32),
        V((4, 8, 128), F32), V((4, 8, 128), F32), V((4, 8, 128), F32), V((2, 8, 128), F32), V((B, 256), F32),
        pltpu.SemaphoreType.DMA((NSEND,)), pltpu.SemaphoreType.DMA((NCOPY,)), pltpu.SemaphoreType.DMA((8,)),
    ]
    return pl.pallas_call(
        body,
        out_shape=(pltpu.VMEM((B, H), F32), pltpu.VMEM((B, DC), F32)),
        in_specs=[pl.BlockSpec(memory_space=pl.ANY)] * 2,
        out_specs=(pl.BlockSpec(memory_space=pltpu.VMEM), pl.BlockSpec(memory_space=pltpu.VMEM)),
        scratch_shapes=scratch,
        compiler_params=pltpu.CompilerParams(
            collective_id=0, has_side_effects=True, vmem_limit_bytes=57 * 1024 * 1024),
    )(grams, weights)


def solution(mesh):
    torus = Mesh(mesh.devices.reshape(mesh.shape["task"], 4, 4, 4), ("task",) + ROW)
    return jax.shard_map(
        per_device, mesh=torus, in_specs=(P("task", ROW, None), P("task", ROW, None)),
        out_specs=(P(ROW, None), P(ROW, None)), check_vma=False)
```
